128 devices in a mesh: rep: 1, r: 4 (over x), s: 32 (over y, z, core).
Axes of the slice: x: 4, y: 4, z: 4, core: 2. Of those that a mesh axis runs over, the one named last changes fastest.
Arguments:
- x: bfloat16 [128, 2048, 1280], P(('rep', 'r', 's'))
- dy: bfloat16 [128, 2048, 1280], P(('rep', 'r', 's'))
- w_gate: bfloat16 [2, 1280, 4480], P(None, 's')
- w_up: bfloat16 [2, 1280, 4480], P(None, 's')
- w_down: bfloat16 [2, 4480, 1280], P(None, 's')
- m_w_gate: float32 [2, 1280, 4480], P(None, 's')
- m_w_up: float32 [2, 1280, 4480], P(None, 's')
- m_w_down: float32 [2, 4480, 1280], P(None, 's')
- v_w_gate: float32 [2, 1280, 4480], P(None, 's')
- v_w_up: float32 [2, 1280, 4480], P(None, 's')
- v_w_down: float32 [2, 4480, 1280], P(None, 's')
Outputs:
- output 1: bfloat16 [2, 1280, 4480], P('rep', 's')
- output 2: bfloat16 [2, 1280, 4480], P('rep', 's')
- output 3: bfloat16 [2, 4480, 1280], P('rep', 's')
- output 4: float32 [2, 1280, 4480], P('rep', 's')
- output 5: float32 [2, 1280, 4480], P('rep', 's')
- output 6: float32 [2, 4480, 1280], P('rep', 's')
- output 7: float32 [2, 1280, 4480], P('rep', 's')
- output 8: float32 [2, 1280, 4480], P('rep', 's')
- output 9: float32 [2, 4480, 1280], P('rep', 's')
All inputs are finite; a program needn't handle non-finite values.
Results may differ from the reference program's by a relative error of at most 0.022.
Values are sent between devices in bfloat16 or wider.
A program may use at most 1.5 GiB of HBM per device.

```python
import jax
import jax.numpy as jnp
from jax import lax

SEQUENCES = 128
TOKENS = 2048
D = 1280
FF = 4480
LAYERS = 2
NAMES = ("w_gate", "w_up", "w_down")
SHAPES = {"w_gate": (LAYERS, D, FF), "w_up": (LAYERS, D, FF), "w_down": (LAYERS, FF, D)}


def bump(key, n, height):
    away = (jnp.arange(n, dtype=jnp.int32) - jax.random.randint(key, (), 0, n, jnp.int32)) % n
    return jnp.where(away < n // 8, height, 1.0)


def together(key, own, strength):
    shared = jax.random.normal(key, own.shape[1:], jnp.float32)
    return (own + strength * shared) * lax.rsqrt(1 + strength * strength)


def setup_inputs(seed: int = 0, part: int = 0) -> dict:
    kx, kdy, ka, kb, kz, kf, kh, kl, *keys = jax.random.split(jax.random.key(seed), 8 + 3 * len(NAMES))
    kx, kdy, ka, kb = (jax.random.fold_in(k, part) for k in (kx, kdy, ka, kb))
    kw, km, kv = (keys[i::3] for i in range(3))
    shape = (SEQUENCES, TOKENS, D)
    much_x, much_dy = jax.random.uniform(kz, (2,), jnp.float32, 0.0, 1.0)
    loud = 2.0 ** jax.random.uniform(jax.random.fold_in(kz, 1), (), jnp.float32, -1.0, 2.0)
    layers = 2.0 ** jax.random.uniform(kl, (LAYERS, 1, 1), jnp.float32, -1.0, 1.0)
    x = together(ka, jax.random.normal(kx, shape, jnp.float32), much_x) * bump(kf, D, 4.0)
    dy = together(kb, jax.random.normal(kdy, shape, jnp.float32), much_dy)
    drawn = {"x": x.astype(jnp.bfloat16), "dy": (loud * dy * (SEQUENCES * TOKENS) ** -0.5).astype(jnp.bfloat16)}
    for key, name in zip(kw, NAMES, strict=True):
        w = jax.random.normal(key, SHAPES[name], jnp.float32) * SHAPES[name][1] ** -0.5
        drawn[name] = (w * {"w_gate": 1.0, "w_up": bump(kh, FF, 4.0), "w_down": layers}[name]).astype(jnp.bfloat16)
    for key, name in zip(km, NAMES, strict=True):
        drawn[f"m_{name}"] = 0.1 * jax.random.normal(key, SHAPES[name], jnp.float32)
    for key, name in zip(kv, NAMES, strict=True):
        drawn[f"v_{name}"] = loud * loud * jax.random.uniform(key, SHAPES[name], jnp.float32, 0.05, 0.15)
    return drawn


def matmul(a, w):
    return jnp.dot(a, w, preferred_element_type=jnp.float32).astype(jnp.bfloat16)


def normed(h):
    wide = h.astype(jnp.float32)
    scale = lax.rsqrt(jnp.mean(wide**2, -1, keepdims=True) + 1e-6)
    return (wide * scale).astype(jnp.bfloat16)


def layer(h, w):
    a = normed(h)
    gate = jnp.dot(a, w["w_gate"], preferred_element_type=jnp.float32)
    up = jnp.dot(a, w["w_up"], preferred_element_type=jnp.float32)
    return h + matmul((jax.nn.silu(gate) * up).astype(jnp.bfloat16), w["w_down"])


def adamw(w, m, v, g):
    m = 0.9 * m + 0.1 * g
    v = 0.95 * v + 0.05 * g * g
    step = m * lax.rsqrt(v + 1e-8) + 0.1 * w
    return (w - 0.02 * step).astype(jnp.bfloat16), m, v


def stack(weights, h):
    return lax.scan(lambda h, w: (layer(h, w), None), h, weights)[0]


def reference(x, dy, w_gate, w_up, w_down, m_w_gate, m_w_up, m_w_down, v_w_gate, v_w_up, v_w_down):
    weights = dict(zip(NAMES, (w_gate, w_up, w_down), strict=True))

    def take(so_far, sequence):
        h, by_y = sequence
        _, back = jax.vjp(lambda w: stack(w, h), weights)
        return jax.tree.map(lambda total, term: total + term.astype(jnp.float32), so_far, back(by_y)[0]), None

    none_yet = {name: jnp.zeros(w.shape, jnp.float32) for name, w in weights.items()}
    by_weights, _ = lax.scan(take, none_yet, (x, dy))
    gradients = [by_weights[name].astype(jnp.bfloat16).astype(jnp.float32) for name in NAMES]
    new = [
        adamw(w.astype(jnp.float32), m, v, g)
        for w, m, v, g in zip((w_gate, w_up, w_down), (m_w_gate, m_w_up, m_w_down), (v_w_gate, v_w_up, v_w_down), gradients, strict=True)
    ]
    return tuple(one[which] for which in range(3) for one in new)
```

```python
import functools

import jax
import jax.numpy as jnp
from jax import lax
from jax.experimental import pallas as pl
from jax.experimental.pallas import tpu as pltpu
from jax.sharding import PartitionSpec as P

NAMES = ("w_gate", "w_up", "w_down")
MESH = pl.DeviceIdType.MESH
F32, BF16 = jnp.float32, jnp.bfloat16


def matmul(a, w):
    return jnp.dot(a, w, preferred_element_type=jnp.float32).astype(jnp.bfloat16)


def normed(h):
    wide = h.astype(jnp.float32)
    scale = lax.rsqrt(jnp.mean(wide**2, -1, keepdims=True) + 1e-6)
    return (wide * scale).astype(jnp.bfloat16)


def adamw(w, m, v, g):
    m = 0.9 * m + 0.1 * g
    v = 0.95 * v + 0.05 * g * g
    step = m * lax.rsqrt(v + 1e-8) + 0.1 * w
    return (w - 0.02 * step).astype(jnp.bfloat16), m, v


WIDE, TALL = "wide", "tall"
QUARTER = {WIDE: (40, 1152), TALL: (72, 640)}


def quarter_of(kind, grad, y, z, c, q):
    if kind == WIDE:
        return grad.at[y, z, pl.ds(pl.multiple_of(40 * c, 8), 40), pl.ds(1152 * q, 1152 if q < 3 else 1024)]
    return grad.at[y, z, pl.ds(72 * q, 72 if q < 3 else 64), pl.ds(pl.multiple_of(640 * c, 128), 640)]


def filled(kind, buffer, q):
    if q < 3:
        return buffer
    return buffer.at[:, :, pl.ds(0, 1024)] if kind == WIDE else buffer.at[:, pl.ds(0, 64), :]


def place():
    s = lax.axis_index("s")
    return lax.axis_index("r"), s // 8, (s // 2) % 4, s % 2


def chip(y, z, c):
    return {"s": (y * 4 + z) * 2 + c}


def turned(u, by):
    return (u + by) % 4


def remote(src, dst, sems, k, where):
    return pltpu.make_async_remote_copy(
        src_ref=src, dst_ref=dst, send_sem=sems[0].at[k], recv_sem=sems[1].at[k], device_id=where, device_id_type=MESH
    )


def added(*terms):
    total = terms[0].astype(F32)
    for term in terms[1:]:
        total = total + term.astype(F32)
    return total.astype(BF16)


def greet():
    x, y, z, c = place()
    others = [chip(y, z, 1 - c), chip(turned(y, 1), z, c), chip(turned(y, 3), z, c), chip(y, turned(z, 1), c), chip(y, turned(z, 3), c)]
    others += [{"r": turned(x, by)} for by in (1, 2, 3)]
    barrier = pltpu.get_barrier_semaphore()
    for other in others:
        pl.semaphore_signal(barrier, inc=1, device_id=other, device_id_type=MESH)
    pl.semaphore_wait(barrier, len(others))


class First:
    ORDER = (2, 1, 3, 0)

    def __init__(self, kind):
        self.kind, (rows, cols) = kind, QUARTER[kind]
        self.scratch = [
            pltpu.VMEM((4, 4, 4, rows, cols), BF16),
            pltpu.VMEM((4, 4, 4, rows, cols), BF16),
            pltpu.VMEM((2, 2, 4, rows, cols), BF16),
            pltpu.VMEM((2, 2, 2, 4, rows, cols), BF16),
            pltpu.SemaphoreType.DMA((16,)),
            pltpu.SemaphoreType.DMA((16,)),
            pltpu.SemaphoreType.DMA((16,)),
            pltpu.SemaphoreType.DMA((4,)),
            pltpu.SemaphoreType.DMA((4,)),
            pltpu.SemaphoreType.DMA((8,)),
            pltpu.SemaphoreType.DMA((8,)),
        ]
        self.out = jax.ShapeDtypeStruct((2, 2, 4, rows, cols), BF16)

    def bind(self, grad, out, refs):
        self.grad, self.out_ref = grad, out
        self.sums, self.theirs, self.near, self.far, self.load, *sems = refs
        self.swap, self.one, self.two = sems[0:2], sems[2:4], sems[4:6]

    def copies0(self, turn, p, j, c, mine):
        _, y, z, _ = place()
        k, q = (turn * 2 + p) * 2 + j, 2 * p + j
        at = turned(y if p == 0 else z, turn)
        part = quarter_of(self.kind, self.grad, *((at, slice(None)) if p == 0 else (slice(None), at)), c, q)
        into = filled(self.kind, (self.sums if mine else self.theirs).at[q, at], q)
        if mine:
            return pltpu.make_async_copy(part, into, self.load.at[k])
        return remote(part, into, self.swap, k, chip(y, z, 1 - place()[3]))

    def neighbours(self, p):
        _, y, z, c = place()
        if p == 0:
            return y, (chip(turned(y, 1), z, c), chip(turned(y, 3), z, c))
        return z, (chip(y, turned(z, 1), c), chip(y, turned(z, 3), c))

    def copy1(self, p, d):
        u, to = self.neighbours(p)
        return remote(self.sums.at[2 * p + d, turned(u, 2)], self.near.at[p, d], self.one, 2 * p + d, to[d])

    def copy2(self, p, d, j):
        u, to = self.neighbours(p)
        return remote(self.sums.at[2 * p + j, turned(u, (1, 3)[d])], self.far.at[p, d, j], self.two, 4 * p + 2 * d + j, to[d])

    def start(self):
        c = place()[3]
        for turn in self.ORDER:
            for p in range(2):
                for j in range(2):
                    self.copies0(turn, p, j, 1 - c, False).start()
                    self.copies0(turn, p, j, c, True).start()

    def pair(self, *turns):
        c = place()[3]
        for turn in turns:
            for p in range(2):
                for j in range(2):
                    self.copies0(turn, p, j, c, True).wait()
                    self.copies0(turn, p, j, 1 - c, False).wait_recv()
        for turn in turns:
            for p in range(2):
                at = turned(self.neighbours(p)[0], turn)

                def one(i, _, p=p, at=at):
                    for j in range(2):
                        q = 2 * p + j
                        self.sums[q, at, i] = added(self.sums[q, at, i], self.theirs[q, at, i])
                    return 0

                lax.fori_loop(0, 4, one, 0)

    def send1(self):
        for p in range(2):
            for d in range(2):
                self.copy1(p, d).start()

    def send2(self):
        for p in range(2):
            for d in range(2):
                self.copy1(p, d).wait_recv()
        for p in range(2):
            u = self.neighbours(p)[0]

            def one(i, _, p=p, u=u):
                for d in range(2):
                    at = turned(u, (1, 3)[d])
                    self.sums[2 * p + d, at, i] = added(self.sums[2 * p + d, at, i], self.near[p, d, i])
                return 0

            lax.fori_loop(0, 4, one, 0)
        for p in range(2):
            for d in range(2):
                for j in range(2):
                    self.copy2(p, d, j).start()

    def finish(self):
        for p in range(2):
            for d in range(2):
                for j in range(2):
                    self.copy2(p, d, j).wait_recv()
        for p in range(2):
            u = self.neighbours(p)[0]

            def one(i, _, p=p, u=u):
                for j in range(2):
                    self.out_ref[p, j, i] = added(self.sums[2 * p + j, u, i], self.far[p, 0, j, i], self.far[p, 1, j, i])
                return 0

            lax.fori_loop(0, 4, one, 0)
        c = place()[3]
        for p in range(2):
            for d in range(2):
                self.copy1(p, d).wait_send()
                for j in range(2):
                    self.copy2(p, d, j).wait_send()
        for turn in self.ORDER:
            for p in range(2):
                for j in range(2):
                    self.copies0(turn, p, j, 1 - c, False).wait_send()

    def slots(self):
        return {0: [self.start], 2: [functools.partial(self.pair, 2), self.send1], 4: [functools.partial(self.pair, 1, 3)], 5: [functools.partial(self.pair, 0)], 7: [self.send2], 99: [self.finish]}


class Second:
    def __init__(self, kind):
        rows, cols = QUARTER[kind]
        self.part = jax.ShapeDtypeStruct((2, 2, 4, rows, cols), BF16)
        self.out = jax.ShapeDtypeStruct((4, rows, cols), BF16)
        self.scratch = [
            pltpu.VMEM((2, 2, rows, cols), BF16),
            pltpu.VMEM((2, 2, 2, rows, cols), BF16),
            pltpu.VMEM((2, 2, 2, rows, cols), BF16),
            pltpu.VMEM((4, rows, cols), BF16),
            pltpu.VMEM((4, rows, cols), BF16),
            pltpu.VMEM((4, rows, cols), BF16),
            pltpu.SemaphoreType.DMA((4,)),
            pltpu.SemaphoreType.DMA((4,)),
            pltpu.SemaphoreType.DMA((4,)),
            pltpu.SemaphoreType.DMA((4,)),
            pltpu.SemaphoreType.DMA((3,)),
            pltpu.SemaphoreType.DMA((3,)),
            pltpu.SemaphoreType.DMA((3,)),
            pltpu.SemaphoreType.DMA((3,)),
        ]

    def bind(self, part, out, refs):
        self.part_ref, self.out_ref = part, out
        self.near, self.far, self.onward, self.block, self.copies, self.whole, *sems = refs
        self.one, self.two, self.cut, self.join = sems[0:2], sems[2:4], sems[4:6], sems[6:8]

    def neighbours(self, p):
        _, y, z, c = place()
        if p == 1:
            return y, (chip(turned(y, 1), z, c), chip(turned(y, 3), z, c))
        return z, (chip(y, turned(z, 1), c), chip(y, turned(z, 3), c))

    def copy1(self, p, d):
        u, to = self.neighbours(p)
        return remote(self.part_ref.at[p, d, turned(u, 2)], self.near.at[p, d], self.one, 2 * p + d, to[d])

    def copy2(self, p, d):
        return remote(self.onward.at[p, d], self.far.at[p, d], self.two, 2 * p + d, self.neighbours(p)[1][d])

    def copy3(self, by):
        x = place()[0]
        return remote(self.block.at[turned(x, by)], self.copies.at[x], self.cut, by - 1, {"r": turned(x, by)})

    def copy4(self, by):
        x = place()[0]
        return remote(self.whole.at[x], self.whole.at[x], self.join, by - 1, {"r": turned(x, by)})

    def start(self):
        for p in range(2):
            for d in range(2):
                self.copy1(p, d).start()

    def send2(self):
        for p in range(2):
            for d in range(2):
                self.copy1(p, d).wait_recv()
        for p in range(2):
            u = self.neighbours(p)[0]
            for d in range(2):
                at = turned(u, (1, 3)[d])
                self.onward[p, d, d] = added(self.part_ref[p, d, at], self.near[p, d])
                self.onward[p, d, 1 - d] = self.part_ref[p, 1 - d, at]
        for p in range(2):
            for d in range(2):
                self.copy2(p, d).start()

    def send3(self):
        for p in range(2):
            for d in range(2):
                self.copy2(p, d).wait_recv()
        for p in range(2):
            u = self.neighbours(p)[0]
            for j in range(2):
                self.block[2 * p + j] = added(self.part_ref[p, j, u], self.far[p, 0, j], self.far[p, 1, j])
        for by in (1, 2, 3):
            self.copy3(by).start()
        x = place()[0]
        self.copies[x] = self.block[x]

    def send4(self):
        for by in (1, 2, 3):
            self.copy3(by).wait_recv()
        x = place()[0]
        self.whole[x] = added(*(self.copies[i] for i in range(4)))
        for by in (1, 2, 3):
            self.copy4(by).start()

    def finish(self):
        for by in (1, 2, 3):
            self.copy4(by).wait_recv()
        self.out_ref[...] = self.whole[...]
        for p in range(2):
            for d in range(2):
                self.copy1(p, d).wait_send()
                self.copy2(p, d).wait_send()
        for by in (1, 2, 3):
            self.copy3(by).wait_send()
            self.copy4(by).wait_send()

    def slots(self):
        return {0: [self.start], 2: [self.send2], 5: [self.send3], 9: [self.send4], 12: [self.finish]}


TILE = 640


def travel(name, number, first, grad, second, part, product=None):
    jobs, inputs, in_specs, outs, out_specs, scratch = [], [], [], [], [], []
    whole = lambda shape: pl.BlockSpec(shape, lambda *_: (0,) * len(shape))
    grid, steps, extra = (1,), 1, {}
    if product is not None:
        lhs, rhs = product
        tall = lhs.shape[1] > rhs.shape[1]
        grid, steps = (7, 2), 14
        depth = lhs.shape[0]
        moving = pl.BlockSpec((depth, TILE), lambda i, j: (0, i))
        still = pl.BlockSpec((depth, 2 * TILE), lambda i, j: (0, 0))
        inputs += [lhs, rhs]
        in_specs += [moving, still] if tall else [still, moving]
        outs.append(jax.ShapeDtypeStruct((lhs.shape[1], rhs.shape[1]), BF16))
        out_specs.append(pl.BlockSpec((TILE, TILE), (lambda i, j: (i, j)) if tall else (lambda i, j: (j, i))))
        extra = dict(
            cost_estimate=pl.CostEstimate(
                flops=2 * depth * lhs.shape[1] * rhs.shape[1], bytes_accessed=60_000_000, transcendentals=0
            )
        )
    if first is not None:
        jobs.append((First(first), grad))
    if second is not None:
        jobs.append((Second(second), part))
    for job, source in jobs:
        inputs.append(source)
        in_specs.append(pl.BlockSpec(memory_space=pl.ANY) if isinstance(job, First) else whole(job.part.shape))
        outs.append(job.out)
        out_specs.append(whole(job.out.shape))
        scratch += job.scratch

    def body(*refs):
        n_in, n_out = len(inputs), len(outs)
        ins, results, rest = refs[:n_in], refs[n_in : n_in + n_out], list(refs[n_in + n_out :])
        skip = 0 if product is None else 2
        plan = {}
        for k, (job, _) in enumerate(jobs):
            job.bind(ins[skip + k], results[(0 if product is None else 1) + k], rest[: len(job.scratch)])
            rest = rest[len(job.scratch) :]
            for slot, actions in job.slots().items():
                plan.setdefault(slot, []).extend(actions)

        def act(slot):
            if slot == 0:
                greet()
            for action in plan.get(slot, []):
                action()

        if product is None:
            for slot in sorted(plan):
                act(slot)
            return
        i, j = pl.program_id(0), pl.program_id(1)
        now = i * 2 + j
        for slot in sorted(plan):
            if slot < steps:
                pl.when(now == slot)(functools.partial(act, slot))
        lhs_ref, rhs_ref = ins[:2]
        piece = pl.ds(pl.multiple_of(j * TILE, 128), TILE)
        left, right = (lhs_ref[...], rhs_ref[:, piece]) if tall else (lhs_ref[:, piece], rhs_ref[...])
        results[0][...] = lax.dot_general(left, right, (((0,), (0,)), ((), ())), preferred_element_type=F32).astype(BF16)

        @pl.when(now == steps - 1)
        def _():
            for slot in sorted(plan):
                if slot >= steps:
                    act(slot)

    return pl.pallas_call(
        body,
        out_shape=tuple(outs),
        grid=grid,
        in_specs=in_specs,
        out_specs=tuple(out_specs),
        scratch_shapes=scratch,
        name=name,
        compiler_params=pltpu.CompilerParams(
            collective_id=number,
            has_side_effects=True,
            vmem_limit_bytes=61_000_000,
            dimension_semantics=("arbitrary",) * len(grid),
        ),
        **extra,
    )(*inputs)


def blocks(grad):
    return grad.reshape(4, 4, grad.shape[0] // 16, grad.shape[1])


def wide_gradient(out):
    return jnp.transpose(out, (1, 0, 2)).reshape(40, 4608)[:, :4480]


def tall_gradient(out):
    half = out.reshape(288, 640)[:280]
    other = lax.ppermute(half, "s", [(i, i ^ 1) for i in range(32)])
    c = lax.axis_index("s") % 2
    both = jnp.where(c == 0, jnp.concatenate([half, other], 1), jnp.concatenate([other, half], 1))
    return lax.dynamic_slice(both, (140 * c, 0), (140, 1280))


def solution(mesh):
    def fetched(w, number, name):
        if name == "w_down":
            padded = jnp.pad(w[number], ((0, 4), (0, 0)))
            return lax.all_gather(padded, "s", axis=0)[:, :140].reshape(4480, 1280)
        return lax.all_gather(w[number], "s", axis=0, tiled=True)

    def step(x, dy, *arrays):
        weights, m, v = (arrays[i : i + 3] for i in (0, 3, 6))
        full = [{name: fetched(w, number, name) for name, w in zip(NAMES, weights, strict=True)} for number in range(2)]

        def up_to_hidden(a, w):
            gate = jnp.dot(a, w["w_gate"], preferred_element_type=F32)
            up = jnp.dot(a, w["w_up"], preferred_element_type=F32)
            return (jax.nn.silu(gate) * up).astype(BF16), (gate, up)

        def split(gate, up, by_hidden):
            _, back = jax.vjp(lambda gate, up: (jax.nn.silu(gate) * up).astype(BF16), gate, up)
            by_gate, by_up = back(by_hidden)
            return by_gate.astype(BF16), by_up.astype(BF16)

        h0, by_y = x[0], dy[0]
        a0 = normed(h0)
        hid0, pre0 = up_to_hidden(a0, full[0])
        h1 = h0 + matmul(hid0, full[0]["w_down"])
        a1, back_norm = jax.vjp(normed, h1)
        hid1, pre1 = up_to_hidden(a1, full[1])

        transposed = lambda g, w: lax.dot_general(g, w, (((1,), (1,)), ((), ())), preferred_element_type=F32)
        by_hid1 = transposed(by_y, full[1]["w_down"]).astype(BF16)
        by_gate1, by_up1 = split(*pre1, by_hid1)
        d1 = lax.dot_general(hid1, by_y, (((0,), (0,)), ((), ())), preferred_element_type=F32).astype(BF16)
        g1, part_d1 = travel("g1", 1, TALL, blocks(d1), None, None, (a1, by_gate1))
        u1, part_g1, sum_d1 = travel("u1", 2, WIDE, blocks(g1), TALL, part_d1, (a1, by_up1))
        by_a1 = transposed(by_gate1, full[1]["w_gate"]).astype(BF16) + transposed(by_up1, full[1]["w_up"]).astype(BF16)
        by_h1 = by_y + back_norm(by_a1)[0]
        by_hid0 = transposed(by_h1, full[0]["w_down"]).astype(BF16)
        by_gate0, by_up0 = split(*pre0, by_hid0)
        d0, part_u1, sum_g1 = travel("d0", 3, WIDE, blocks(u1), WIDE, part_g1, (hid0, by_h1))
        g0, part_d0, sum_u1 = travel("g0", 4, TALL, blocks(d0), WIDE, part_u1, (a0, by_gate0))
        u0, part_g0, sum_d0 = travel("u0", 5, WIDE, blocks(g0), TALL, part_d0, (a0, by_up0))
        part_u0, sum_g0 = travel("t0", 6, WIDE, blocks(u0), WIDE, part_g0)
        (sum_u0,) = travel("t1", 7, None, None, WIDE, part_u0)
        gradients = [
            jnp.stack([wide_gradient(sum_g0), wide_gradient(sum_g1)]),
            jnp.stack([wide_gradient(sum_u0), wide_gradient(sum_u1)]),
            jnp.stack([tall_gradient(sum_d0), tall_gradient(sum_d1)]),
        ]
        new = [adamw(w.astype(F32), m, v, g.astype(F32)) for w, m, v, g in zip(weights, m, v, gradients, strict=True)]
        return tuple(one[which] for which in range(3) for one in new)

    states, cut = P(("rep", "r", "s"), None, None), P(None, "s", None)
    return jax.shard_map(
        step,
        mesh=mesh,
        in_specs=(states, states) + (cut,) * 9,
        out_specs=(P("rep", "s", None),) * 9,
        check_vma=False,
    )
```
